512 devices in a mesh: fsdp: 128 (over x, z, core), grp: 4 (over y).
Axes of the slice: x: 4, y: 4, z: 16, core: 2. Of those that a mesh axis runs over, the one named last changes fastest.
Arguments:
- grad: bfloat16 [28672, 8192], P('fsdp', 'grp'), may hold values from -6 to 6
- projector_t: bfloat16 [1024, 8192], P('fsdp', 'grp'), may hold values from -0.0625 to 0.0625
- first_moment: float32 [28672, 1024], P('fsdp', 'grp'), may hold values from -3 to 3
- second_moment: float32 [28672, 1024], P('fsdp', 'grp'), may hold values from 0.0001 to 0.01
Outputs:
- update: float32 [28672, 8192], P('fsdp', 'grp')
- first_new: float32 [28672, 1024], P('fsdp', 'grp')
- second_new: float32 [28672, 1024], P('fsdp', 'grp')
The draws below stay inside these ranges and needn't reach their ends.
All inputs are finite; a program needn't handle non-finite values.
Results may differ from the reference program's by a relative error of at most 0.0029.
Values may be sent and summed in bfloat16 or wider, within the bound.
No kernel may reach another device: no remote copies, remote signals or barrier semaphores. Data moves between devices by JAX's collectives and lax.ppermute only.
A program may use at most 64 MiB of HBM per device.

```python
import math
import jax
import jax.numpy as jnp
from jax import lax

M = 8192
N = 28672
R = 1024
STEP = 10


def steps_of(own_key, extent, split, least, largest):
    level = 1.0
    for axis_at, parts in split:
        draws = jax.random.uniform(jax.random.fold_in(jax.random.fold_in(own_key, 6), axis_at), (parts,), jnp.float32, least / len(split), largest / len(split))
        level = level * jnp.repeat(jnp.exp(draws), extent[axis_at] // parts).reshape((-1,) + (1,) * (len(extent) - 1 - axis_at))
    return level


def centred(rng, dims, spread, most, cuts=(), held_as=jnp.bfloat16):
    values = spread * jax.random.normal(rng, dims, jnp.float32)
    if cuts:
        values = values * steps_of(rng, dims, cuts, -0.22, 0.18)
    return jnp.clip(values, -most, most).astype(held_as)


def setup_inputs(seed: int = 0) -> dict:
    splits = jax.random.split(jax.random.key(seed), 5)
    return {
        "grad": centred(splits[0], (N, M), 1.0, 6.0, ((0, 128), (1, 4))),
        "projector_t": centred(splits[1], (R, M), M ** -0.5, 0.0625, ((0, 128), (1, 4))),
        "first_moment": centred(splits[2], (N, R), 0.5, 3.0, ((0, 128), (1, 4)), jnp.float32),
        "second_moment": jnp.clip(jnp.exp(math.log(0.01) - 4.6051702 * jax.random.uniform(splits[3], (N, R), jnp.float32) ** steps_of(splits[3], (N, R), ((0, 128), (1, 4)), -0.2, 0.2)), 0.0001, 0.01),
    }


def reference(grad, projector_t, first_moment, second_moment):
    projected = lax.dot_general(grad, projector_t, (((1,), (1,)), ((), ())), preferred_element_type=jnp.float32)
    first_new = 0.9 * first_moment + 0.1 * projected
    second_new = 0.999 * second_moment + 0.001 * projected * projected
    correct_one = 1.0 - 0.9 ** STEP
    correct_two = 1.0 - 0.999 ** STEP
    normalized = (first_new / correct_one / (jnp.sqrt(second_new / correct_two) + 1e-08)).astype(jnp.bfloat16)
    update = jnp.dot(normalized, projector_t, preferred_element_type=jnp.float32)
    return (update, first_new, second_new)
```

```python
import jax
import jax.numpy as jnp
from jax import lax
from jax.sharding import PartitionSpec as P

STEP = 10


def body(grad, projector_t, first_moment, second_moment):
    whole = lax.all_gather(projector_t, "fsdp", axis=0, tiled=True)
    partial_value = lax.dot_general(
        grad, whole, (((1,), (1,)), ((), ())), preferred_element_type=jnp.float32
    )
    parts = jnp.moveaxis(partial_value.reshape(partial_value.shape[0], 4, -1), 1, 0)
    projected = jnp.sum(lax.all_to_all(parts, "grp", 0, 0, tiled=True), axis=0)
    first_new = 0.9 * first_moment + 0.1 * projected
    second_new = 0.999 * second_moment + 0.001 * projected * projected
    correct_one = 1.0 - 0.9**STEP
    correct_two = 1.0 - 0.999**STEP
    normalized = (first_new / correct_one / (jnp.sqrt(second_new / correct_two) + 1e-08)).astype(
        jnp.bfloat16
    )
    full_step = lax.all_to_all(
        jnp.broadcast_to(normalized[None], (4, *normalized.shape)), "grp", 0, 0, tiled=True
    )
    full_step = jnp.moveaxis(full_step, 0, 1).reshape(normalized.shape[0], -1)
    update = jnp.dot(full_step, whole, preferred_element_type=jnp.float32)
    return (update, first_new, second_new)


def solution(mesh):
    spec = P("fsdp", "grp")
    return jax.shard_map(
        body, mesh=mesh, in_specs=(spec,) * 4, out_specs=(spec,) * 3, check_vma=False
    )
```

```python
import jax
import jax.numpy as jnp
from jax import lax
from jax.sharding import Mesh
from jax.sharding import PartitionSpec as P

STEP = 10
FSDP = ("x", "z", "c")


def copies(shard, axis):
    peers = lax.axis_size(axis)
    return lax.all_to_all(
        jnp.broadcast_to(shard[None], (peers, *shard.shape)), axis, 0, 0, tiled=True
    )


def body(grad, projector_t, first_moment, second_moment):
    parts = copies(projector_t, "z")
    parts = copies(parts, "x")
    parts = copies(parts, "c")
    whole = parts.transpose(1, 2, 0, 3, 4)
    blocks = whole.reshape(4, 256, -1)
    partial_value = lax.dot_general(
        blocks, grad, (((2,), (1,)), ((), ())), preferred_element_type=jnp.float32
    ).transpose(0, 2, 1)
    projected = jnp.sum(lax.all_to_all(partial_value, "y", 0, 0, tiled=True), axis=0)
    first_new = 0.9 * first_moment + 0.1 * projected
    second_new = 0.999 * second_moment + 0.001 * projected * projected
    correct_one = 1.0 - 0.9**STEP
    correct_two = 1.0 - 0.999**STEP
    normalized = (first_new / correct_one / (jnp.sqrt(second_new / correct_two) + 1e-08)).astype(
        jnp.bfloat16
    )
    full_step = jnp.moveaxis(copies(normalized, "y"), 0, 1).reshape(normalized.shape[0], -1)
    update = jnp.dot(full_step, whole.reshape(1024, -1), preferred_element_type=jnp.float32)
    return (update, first_new, second_new)


def solution(mesh):
    finer = Mesh(mesh.devices.reshape(4, 16, 2, 4), ("x", "z", "c", "y"))
    spec = P(FSDP, "y")
    return jax.shard_map(
        body, mesh=finer, in_specs=(spec,) * 4, out_specs=(spec,) * 3, check_vma=False
    )
```

```python
import jax
import jax.numpy as jnp
from jax import lax
from jax.experimental import pallas as pl
from jax.experimental.pallas import tpu as pltpu
from jax.sharding import Mesh
from jax.sharding import PartitionSpec as P

STEP = 10
FSDP = ("x", "z", "c")
VMEM = pl.BlockSpec(memory_space=pltpu.VMEM)
ROTATED = [[4 * x + (x + d) % 4 for d in range(4)] for x in range(4)]


def exchange(parts):
    return lax.all_to_all(parts, ("x", "y"), 0, 0, axis_index_groups=ROTATED, tiled=True)


def project_some(slots, grad, pieces, out):
    for at, slot in enumerate(slots):
        rows = jnp.concatenate([pieces[2 * at][...], pieces[2 * at + 1][...]], axis=0)
        out[slot] = lax.dot_general(
            grad[...], rows, (((1,), (1,)), ((), ())), preferred_element_type=jnp.float32
        ).astype(jnp.bfloat16)


def first_projection(grad, *refs):
    project_some((0, 1, 3), grad, refs[:-1], refs[-1])


def last_projection(grad, own, other, before, out):
    for k in (0, 1, 3):
        out[k] = before[k]
    project_some((2,), grad, (own, other), out)


def moments(core, received, first, second, first_out, second_out, copies):
    at = lax.broadcasted_iota(jnp.int32, (256, 256), 0)
    rank = lax.broadcasted_iota(jnp.int32, (256, 256), 1)
    half = jnp.bitwise_xor(lax.shift_right_logical(at, 7), core[0])
    spot = (lax.shift_right_logical(at, 3) & 15) * 16 + half * 8 + (at & 7)
    place = (rank == spot).astype(jnp.bfloat16)
    projected = jnp.zeros(first.shape, jnp.float32)
    for k in range(4):
        projected += jnp.dot(received[k], place, preferred_element_type=jnp.float32)
    first_new = 0.9 * first[...] + 0.1 * projected
    second_new = 0.999 * second[...] + 0.001 * projected * projected
    first_out[...] = first_new
    second_out[...] = second_new
    correct_one = 1.0 - 0.9**STEP
    correct_two = 1.0 - 0.999**STEP
    normalized = (first_new / correct_one / (jnp.sqrt(second_new / correct_two) + 1e-08)).astype(
        jnp.bfloat16
    )
    turned = lax.dot_general(
        normalized, place, (((1,), (1,)), ((), ())), preferred_element_type=jnp.float32
    ).astype(jnp.bfloat16)
    for k in range(4):
        copies[k] = turned


def back(steps, *refs):
    pieces, out, held, sems = refs[:8], refs[8], refs[9], refs[10]
    width = 512
    sent = []
    for k in range(4):
        columns = pl.ds(k * width, width)
        total = jnp.zeros((steps.shape[1], width), jnp.float32)
        for d in range(4):
            rows = jnp.concatenate(
                [pieces[2 * d][:, columns], pieces[2 * d + 1][:, columns]], axis=0
            )
            total += jnp.dot(steps[d], rows, preferred_element_type=jnp.float32)
        held[:, columns] = total
        copy = pltpu.make_async_copy(held.at[:, columns], out.at[:, columns], sems.at[k])
        copy.start()
        sent.append(copy)
    for copy in sent:
        copy.wait()


def limit(mib):
    return pltpu.CompilerParams(vmem_limit_bytes=mib * 2**20)


def body(grad, projector_t, first_moment, second_moment):
    own = lax.all_gather(projector_t, "z", axis=0, tiled=True)

    def from_x(d):
        return lax.ppermute(own, "x", [(x, (x - d) % 4) for x in range(4)])

    def from_core(block):
        return lax.ppermute(block, "c", [(0, 1), (1, 0)])

    blocks = {0: own}
    for d in (1, 3, 2):
        blocks[d] = from_x(d)
    others = {d: from_core(blocks[d]) for d in (0, 1, 3, 2)}
    columns, ranks = first_moment.shape
    shape = jax.ShapeDtypeStruct((4, columns, ranks), jnp.bfloat16)
    three = [half[d] for d in (0, 1, 3) for half in (blocks, others)]
    parts = pl.pallas_call(
        first_projection,
        out_shape=shape,
        in_specs=[VMEM] * 7,
        out_specs=VMEM,
        compiler_params=limit(16),
        name="first_projection",
    )(grad, *three)
    parts = pl.pallas_call(
        last_projection,
        out_shape=shape,
        in_specs=[VMEM] * 4,
        out_specs=VMEM,
        compiler_params=limit(16),
        name="last_projection",
    )(grad, blocks[2], others[2], parts)
    received = exchange(parts)
    core = lax.axis_index("c").astype(jnp.int32).reshape(1)
    held = jax.ShapeDtypeStruct(first_moment.shape, jnp.float32)
    first_new, second_new, copies = pl.pallas_call(
        moments,
        out_shape=(held, held, shape),
        in_specs=[pl.BlockSpec(memory_space=pltpu.SMEM)] + [VMEM] * 3,
        out_specs=(VMEM,) * 3,
        compiler_params=limit(16),
        name="moments",
    )(core, received, first_moment, second_moment)
    steps = exchange(copies)
    width = grad.shape[1]
    update = pl.pallas_call(
        back,
        out_shape=jax.ShapeDtypeStruct((columns, width), jnp.float32),
        in_specs=[VMEM] * 9,
        out_specs=pl.BlockSpec(memory_space=pl.ANY),
        scratch_shapes=[pltpu.VMEM((columns, width), jnp.float32), pltpu.SemaphoreType.DMA((4,))],
        compiler_params=limit(16),
        name="back",
    )(steps, *[half[d] for d in range(4) for half in (blocks, others)])
    return (update, first_new, second_new)


def solution(mesh):
    finer = Mesh(mesh.devices.reshape(4, 16, 2, 4), ("x", "z", "c", "y"))
    spec = P(FSDP, "y")
    return jax.shard_map(
        body, mesh=finer, in_specs=(spec,) * 4, out_specs=(spec,) * 3, check_vma=False
    )
```

```python
import jax
import jax.numpy as jnp
from jax import lax
from jax.experimental import pallas as pl
from jax.experimental.pallas import tpu as pltpu
from jax.sharding import Mesh
from jax.sharding import PartitionSpec as P

STEP = 10
FSDP = ("x", "z", "c")
VMEM = pl.BlockSpec(memory_space=pltpu.VMEM)
ROTATED = [[4 * x + (x + d) % 4 for d in range(4)] for x in range(4)]


def exchange(parts):
    return lax.all_to_all(parts, ("x", "y"), 0, 0, axis_index_groups=ROTATED, tiled=True)


def encode(part):
    scaled = part * 2.0**22
    square = scaled * scaled
    return jnp.where(part < 0.0, -square * square, square * square).astype(jnp.bfloat16)


def decode(sent):
    fourth = sent.astype(jnp.float32)
    size = jnp.sqrt(jnp.sqrt(jnp.abs(fourth))) * 2.0**-22
    return jnp.where(fourth < 0.0, -size, size)


def project(grad, own, other):
    rows = jnp.concatenate([own[...], other[...]], axis=0)
    return lax.dot_general(
        grad[...], rows, (((1,), (1,)), ((), ())), preferred_element_type=jnp.float32
    )


def first_block(grad, first, second, own, other, part):
    part[...] = project(grad, own, other)


def middle_blocks(grad, own_1, other_1, own_3, other_3, part_1, part_3):
    part_1[...] = project(grad, own_1, other_1)
    part_3[...] = project(grad, own_3, other_3)


def last_block(grad, own, other, part_0, part_1, part_3, out):
    parts = [part_0[...], part_1[...], project(grad, own, other), part_3[...]]
    for k in range(4):
        out[k] = encode(parts[k])


def moments(received, first, second, first_out, second_out, copies):
    at = lax.broadcasted_iota(jnp.int32, (256, 256), 0)
    rank = lax.broadcasted_iota(jnp.int32, (256, 256), 1)
    half = jnp.bitwise_xor(lax.shift_right_logical(at, 7), lax.axis_index("c"))
    spot = (lax.shift_right_logical(at, 3) & 15) * 16 + half * 8 + (at & 7)
    place = (rank == spot).astype(jnp.bfloat16)
    left = decode(received[0])
    for k in (1, 2, 3):
        left += decode(received[k])
    projected = jnp.zeros(first.shape, jnp.float32)
    for _ in range(3):
        piece = left.astype(jnp.bfloat16)
        projected += jnp.dot(piece, place, preferred_element_type=jnp.float32)
        left = left - piece.astype(jnp.float32)
    first_new = 0.9 * first[...] + 0.1 * projected
    second_new = 0.999 * second[...] + 0.001 * projected * projected
    first_out[...] = first_new
    second_out[...] = second_new
    correct_one = 1.0 - 0.9**STEP
    correct_two = 1.0 - 0.999**STEP
    normalized = (first_new / correct_one / (jnp.sqrt(second_new / correct_two) + 1e-08)).astype(
        jnp.bfloat16
    )
    turned = lax.dot_general(
        normalized, place, (((1,), (1,)), ((), ())), preferred_element_type=jnp.float32
    ).astype(jnp.bfloat16)
    for k in range(4):
        copies[k] = turned


def back(steps, *refs):
    pieces, out, held, sems = refs[:8], refs[8], refs[9], refs[10]
    width = 512
    sent = []
    for k in range(4):
        columns = pl.ds(k * width, width)
        total = jnp.zeros((steps.shape[1], width), jnp.float32)
        for d in range(4):
            rows = jnp.concatenate(
                [pieces[2 * d][:, columns], pieces[2 * d + 1][:, columns]], axis=0
            )
            total += jnp.dot(steps[d], rows, preferred_element_type=jnp.float32)
        held[:, columns] = total
        copy = pltpu.make_async_copy(held.at[:, columns], out.at[:, columns], sems.at[k])
        copy.start()
        sent.append(copy)
    for copy in sent:
        copy.wait()


def limit(mib):
    return pltpu.CompilerParams(vmem_limit_bytes=mib * 2**20)


def body(grad, projector_t, first_moment, second_moment):
    own = lax.all_gather(projector_t, "z", axis=0, tiled=True)

    def from_x(d):
        return lax.ppermute(own, "x", [(x, (x - d) % 4) for x in range(4)])

    def from_core(block):
        return lax.ppermute(block, "c", [(0, 1), (1, 0)])

    blocks = {0: own}
    for d in (1, 3, 2):
        blocks[d] = from_x(d)
    others = {d: from_core(blocks[d]) for d in (0, 1, 3, 2)}
    columns, ranks = first_moment.shape
    shape = jax.ShapeDtypeStruct((4, columns, ranks), jnp.bfloat16)
    held = jax.ShapeDtypeStruct(first_moment.shape, jnp.float32)
    part_0 = pl.pallas_call(
        first_block,
        out_shape=held,
        in_specs=[VMEM] * 5,
        out_specs=VMEM,
        compiler_params=limit(8),
        name="first_block",
    )(grad, first_moment, second_moment, blocks[0], others[0])
    part_1, part_3 = pl.pallas_call(
        middle_blocks,
        out_shape=(held, held),
        in_specs=[VMEM] * 5,
        out_specs=(VMEM,) * 2,
        compiler_params=limit(8),
        name="middle_blocks",
    )(grad, blocks[1], others[1], blocks[3], others[3])
    parts = pl.pallas_call(
        last_block,
        out_shape=shape,
        in_specs=[VMEM] * 6,
        out_specs=VMEM,
        compiler_params=limit(8),
        name="last_block",
    )(grad, blocks[2], others[2], part_0, part_1, part_3)
    received = exchange(parts)
    first_new, second_new, copies = pl.pallas_call(
        moments,
        out_shape=(held, held, shape),
        in_specs=[VMEM] * 3,
        out_specs=(VMEM,) * 3,
        compiler_params=limit(8),
        name="moments",
    )(received, first_moment, second_moment)
    steps = exchange(copies)
    width = projector_t.shape[1]
    update = pl.pallas_call(
        back,
        out_shape=jax.ShapeDtypeStruct((columns, width), jnp.float32),
        in_specs=[VMEM] * 9,
        out_specs=pl.BlockSpec(memory_space=pl.ANY),
        scratch_shapes=[pltpu.VMEM((columns, width), jnp.float32), pltpu.SemaphoreType.DMA((4,))],
        compiler_params=limit(8),
        name="back",
    )(steps, *[half[d] for d in range(4) for half in (blocks, others)])
    return (update, first_new, second_new)


def solution(mesh):
    finer = Mesh(mesh.devices.reshape(4, 16, 2, 4), ("x", "z", "c", "y"))
    spec = P(FSDP, "y")
    return jax.shard_map(
        body, mesh=finer, in_specs=(spec,) * 4, out_specs=(spec,) * 3, check_vma=False
    )
```

```python
import jax
import jax.numpy as jnp
from jax import lax
from jax.experimental import pallas as pl
from jax.experimental.pallas import tpu as pltpu
from jax.sharding import Mesh
from jax.sharding import PartitionSpec as P


STEP = 10
FSDP = ("x", "z", "c")
VMEM = pl.BlockSpec(memory_space=pltpu.VMEM)
ROTATED = [[4 * x + (x + d) % 4 for d in range(4)] for x in range(4)]


def exchange(parts):
    return lax.all_to_all(parts, ("x", "y"), 0, 0, axis_index_groups=ROTATED, tiled=True)


def encode(part):
    scaled = part * 2.0**22
    square = scaled * scaled
    return jnp.where(part < 0.0, -square * square, square * square).astype(jnp.bfloat16)


def decode(sent):
    fourth = sent.astype(jnp.float32)
    size = jnp.sqrt(jnp.sqrt(jnp.abs(fourth))) * 2.0**-22
    return jnp.where(fourth < 0.0, -size, size)


def project(grad, own, other):
    rows = jnp.concatenate([own[...], other[...]], axis=0)
    return lax.dot_general(
        grad[...], rows, (((1,), (1,)), ((), ())), preferred_element_type=jnp.float32
    )


def first_block(grad, own, other, part):
    part[...] = encode(project(grad, own, other))


def middle_blocks(grad, own_1, other_1, own_3, other_3, part_1, part_3):
    part_1[...] = encode(project(grad, own_1, other_1))
    part_3[...] = encode(project(grad, own_3, other_3))


def last_block(grad, own, other, part_0, part_1, part_3, out):
    out[0] = part_0[...]
    out[1] = part_1[...]
    out[3] = part_3[...]
    out[2] = encode(project(grad, own, other))


def moments(received, first, second, first_out, second_out, copies):
    at = lax.broadcasted_iota(jnp.int32, (256, 256), 0)
    rank = lax.broadcasted_iota(jnp.int32, (256, 256), 1)
    half = jnp.bitwise_xor(lax.shift_right_logical(at, 7), lax.axis_index("c"))
    spot = (lax.shift_right_logical(at, 3) & 15) * 16 + half * 8 + (at & 7)
    place = (rank == spot).astype(jnp.bfloat16)
    left = decode(received[0])
    for k in (1, 2, 3):
        left += decode(received[k])
    projected = jnp.zeros(first.shape, jnp.float32)
    for _ in range(3):
        piece = left.astype(jnp.bfloat16)
        projected += jnp.dot(piece, place, preferred_element_type=jnp.float32)
        left = left - piece.astype(jnp.float32)
    first_new = 0.9 * first[...] + 0.1 * projected
    second_new = 0.999 * second[...] + 0.001 * projected * projected
    first_out[...] = first_new
    second_out[...] = second_new
    correct_one = 1.0 - 0.9**STEP
    correct_two = 1.0 - 0.999**STEP
    normalized = (first_new / correct_one / (jnp.sqrt(second_new / correct_two) + 1e-08)).astype(
        jnp.bfloat16
    )
    turned = lax.dot_general(
        normalized, place, (((1,), (1,)), ((), ())), preferred_element_type=jnp.float32
    ).astype(jnp.bfloat16)
    for k in range(4):
        copies[k] = turned


def back(steps, first, second, *refs):
    pieces, (out, first_out, second_out, held, sems) = refs[:8], refs[8:]
    width = 512
    sent = [
        pltpu.make_async_copy(first, first_out, sems.at[4]),
        pltpu.make_async_copy(second, second_out, sems.at[5]),
    ]
    for copy in sent:
        copy.start()
    for k in range(4):
        columns = pl.ds(k * width, width)
        total = jnp.zeros((steps.shape[1], width), jnp.float32)
        for d in range(4):
            rows = jnp.concatenate(
                [pieces[2 * d][:, columns], pieces[2 * d + 1][:, columns]], axis=0
            )
            total += jnp.dot(steps[d], rows, preferred_element_type=jnp.float32)
        held[:, columns] = total
        copy = pltpu.make_async_copy(held.at[:, columns], out.at[:, columns], sems.at[k])
        copy.start()
        sent.append(copy)
    for copy in sent:
        copy.wait()


def limit(mib):
    return pltpu.CompilerParams(vmem_limit_bytes=mib * 2**20)


def call(kernel, out_shape, *operands):
    many = isinstance(out_shape, tuple)
    return pl.pallas_call(
        kernel,
        out_shape=out_shape,
        in_specs=[VMEM] * len(operands),
        out_specs=(VMEM,) * len(out_shape) if many else VMEM,
        compiler_params=limit(8),
    )(*operands)


def step(grad, projector_t, first_moment, second_moment):
    own = lax.all_gather(projector_t, "z", axis=0, tiled=True)

    def from_x(d):
        return lax.ppermute(own, "x", [(x, (x - d) % 4) for x in range(4)])

    def from_core(d):
        return lax.ppermute(blocks[d], "c", [(0, 1), (1, 0)])

    blocks = {0: own}
    for d in (1, 3, 2):
        blocks[d] = from_x(d)
    others = {d: from_core(d) for d in (0, 1, 3, 2)}
    columns, ranks = first_moment.shape
    one = jax.ShapeDtypeStruct((columns, ranks), jnp.bfloat16)
    four = jax.ShapeDtypeStruct((4, columns, ranks), jnp.bfloat16)
    held = jax.ShapeDtypeStruct((columns, ranks), jnp.float32)
    part_0 = call(first_block, one, grad, blocks[0], others[0])
    part_1, part_3 = call(
        middle_blocks, (one, one), grad, blocks[1], others[1], blocks[3], others[3]
    )
    parts = call(last_block, four, grad, blocks[2], others[2], part_0, part_1, part_3)
    received = exchange(parts)
    first_new, second_new, copies = call(
        moments, (held, held, four), received, first_moment, second_moment
    )
    steps = exchange(copies)
    width = projector_t.shape[1]
    HBM = pl.BlockSpec(memory_space=pl.ANY)
    return pl.pallas_call(
        back,
        out_shape=(jax.ShapeDtypeStruct((columns, width), jnp.float32), held, held),
        in_specs=[VMEM] * 11,
        out_specs=(HBM,) * 3,
        scratch_shapes=[pltpu.VMEM((columns, width), jnp.float32), pltpu.SemaphoreType.DMA((6,))],
        compiler_params=limit(8),
        name="back",
    )(steps, first_new, second_new, *[half[d] for d in range(4) for half in (blocks, others)])


def solution(mesh):
    finer = Mesh(mesh.devices.reshape(4, 16, 2, 4), ("x", "z", "c", "y"))
    spec = P(FSDP, "y")
    return jax.shard_map(
        step, mesh=finer, in_specs=(spec,) * 4, out_specs=(spec,) * 3, check_vma=False
    )
```

```python
import jax
import jax.numpy as jnp
from jax import lax
from jax.experimental import pallas as pl
from jax.experimental.pallas import tpu as pltpu
from jax.sharding import Mesh
from jax.sharding import PartitionSpec as P


STEP = 10
FSDP = ("x", "z", "c")
VMEM = pl.BlockSpec(memory_space=pltpu.VMEM)
ROTATED = [[4 * x + (x + d) % 4 for d in range(4)] for x in range(4)]
BOTH = [[(2 * x + c) * 4 + (x + d) % 4 for c in range(2) for d in range(4)] for x in range(4)]


def exchange(parts):
    return lax.all_to_all(parts, ("x", "y"), 0, 0, axis_index_groups=ROTATED, tiled=True)


def exchange_both(parts):
    return lax.all_to_all(parts, ("x", "c", "y"), 0, 0, axis_index_groups=BOTH, tiled=True)


def encode(part):
    scaled = part * 2.0**22
    square = scaled * scaled
    return jnp.where(part < 0.0, -square * square, square * square).astype(jnp.bfloat16)


def decode(sent):
    fourth = sent.astype(jnp.float32)
    size = jnp.sqrt(jnp.sqrt(jnp.abs(fourth))) * 2.0**-22
    return jnp.where(fourth < 0.0, -size, size)


def project(own, swapped, rows, parts):
    for k, grad in enumerate((own, swapped)):
        parts[k] = encode(
            lax.dot_general(
                grad[...], rows, (((1,), (1,)), ((), ())), preferred_element_type=jnp.float32
            )
        )


def first_block(own, swapped, rows, parts):
    project(own, swapped, rows[...], parts)


def middle_block(own, swapped, rows, parts):
    project(own, swapped, rows[...], parts)


def last_blocks(own, swapped, rows_1, rows_2, parts_0, parts_3, out, pair, held):
    core = lax.axis_index("c")
    rows = jnp.concatenate([rows_1[...], rows_2[...]], axis=0)
    pair[...] = rows
    project(own, swapped, rows, held)
    for k in range(2):
        slot = 4 * jnp.bitwise_xor(core, k)
        out[slot] = parts_0[k]
        out[slot + 1] = held[k, :, :128]
        out[slot + 2] = held[k, :, 128:]
        out[slot + 3] = parts_3[k]


def moments(received, first, second, first_out, second_out, copies):
    at = lax.broadcasted_iota(jnp.int32, (256, 256), 0)
    rank = lax.broadcasted_iota(jnp.int32, (256, 256), 1)
    core = lax.axis_index("c")
    half = jnp.bitwise_xor(lax.shift_right_logical(at, 7), core)
    spot = (lax.shift_right_logical(at, 3) & 15) * 16 + half * 8 + (at & 7)
    place = (rank == spot).astype(jnp.bfloat16)
    halves = []
    for k in range(2):
        slot = 4 * jnp.bitwise_xor(core, k)
        halves.append(sum(decode(received[slot + d]) for d in range(4)))
    left = jnp.concatenate(halves, axis=1)
    projected = jnp.zeros(first.shape, jnp.float32)
    for _ in range(3):
        piece = left.astype(jnp.bfloat16)
        projected += jnp.dot(piece, place, preferred_element_type=jnp.float32)
        left = left - piece.astype(jnp.float32)
    first_new = 0.9 * first[...] + 0.1 * projected
    second_new = 0.999 * second[...] + 0.001 * projected * projected
    first_out[...] = first_new
    second_out[...] = second_new
    correct_one = 1.0 - 0.9**STEP
    correct_two = 1.0 - 0.999**STEP
    normalized = (first_new / correct_one / (jnp.sqrt(second_new / correct_two) + 1e-08)).astype(
        jnp.bfloat16
    )
    turned = lax.dot_general(
        normalized, place, (((1,), (1,)), ((), ())), preferred_element_type=jnp.float32
    ).astype(jnp.bfloat16)
    for k in range(4):
        copies[k] = turned


def back(steps, first, second, *refs):
    (own_0, other_0, pair, other_pair, own_3, other_3), refs = refs[:6], refs[6:]
    out, first_out, second_out, held, sems = refs
    low, high = pl.ds(0, 128), pl.ds(128, 128)
    width = 512
    sent = [
        pltpu.make_async_copy(first, first_out, sems.at[4]),
        pltpu.make_async_copy(second, second_out, sems.at[5]),
    ]
    for copy in sent:
        copy.start()
    for k in range(4):
        columns = pl.ds(k * width, width)
        total = jnp.zeros((steps.shape[1], width), jnp.float32)
        for d, (one, two, where) in enumerate(
            (
                (own_0, other_0, low),
                (pair, other_pair, low),
                (pair, other_pair, high),
                (own_3, other_3, low),
            )
        ):
            rows = jnp.concatenate([one[where, columns], two[where, columns]], axis=0)
            total += jnp.dot(steps[d], rows, preferred_element_type=jnp.float32)
        held[:, columns] = total
        copy = pltpu.make_async_copy(held.at[:, columns], out.at[:, columns], sems.at[k])
        copy.start()
        sent.append(copy)
    for copy in sent:
        copy.wait()


def limit(mib):
    return pltpu.CompilerParams(vmem_limit_bytes=mib * 2**20)


def call(kernel, out_shape, *operands):
    many = isinstance(out_shape, tuple)
    return pl.pallas_call(
        kernel,
        out_shape=out_shape,
        in_specs=[VMEM] * len(operands),
        out_specs=(VMEM,) * len(out_shape) if many else VMEM,
        compiler_params=limit(8),
    )(*operands)


def step(grad, projector_t, first_moment, second_moment):
    own = lax.all_gather(projector_t, "z", axis=0, tiled=True)

    def from_x(d):
        return lax.ppermute(own, "x", [(x, (x - d) % 4) for x in range(4)])

    def from_core(block):
        return lax.ppermute(block, "c", [(0, 1), (1, 0)])

    blocks = {0: own}
    for d in (1, 3, 2):
        blocks[d] = from_x(d)
    other_0 = from_core(blocks[0])
    other_3 = from_core(blocks[3])
    columns, ranks = first_moment.shape
    two = jax.ShapeDtypeStruct((2, columns, ranks // 2), jnp.bfloat16)
    eight = jax.ShapeDtypeStruct((8, columns, ranks // 2), jnp.bfloat16)
    four = jax.ShapeDtypeStruct((4, columns, ranks), jnp.bfloat16)
    held = jax.ShapeDtypeStruct((columns, ranks), jnp.float32)
    swapped = lax.ppermute(grad, "c", [(0, 1), (1, 0)])
    parts_0 = call(first_block, two, grad, swapped, blocks[0])
    parts_3 = call(middle_block, two, grad, swapped, blocks[3])
    parts, pair = pl.pallas_call(
        last_blocks,
        out_shape=(eight, jax.ShapeDtypeStruct((256, grad.shape[1]), jnp.bfloat16)),
        in_specs=[VMEM] * 6,
        out_specs=(VMEM,) * 2,
        scratch_shapes=[pltpu.VMEM((2, columns, ranks), jnp.bfloat16)],
        compiler_params=limit(8),
        name="last_blocks",
    )(grad, swapped, blocks[1], blocks[2], parts_0, parts_3)
    other_pair = from_core(pair)
    received = exchange_both(parts)
    first_new, second_new, copies = call(
        moments, (held, held, four), received, first_moment, second_moment
    )
    steps = exchange(copies)
    width = projector_t.shape[1]
    HBM = pl.BlockSpec(memory_space=pl.ANY)
    return pl.pallas_call(
        back,
        out_shape=(jax.ShapeDtypeStruct((columns, width), jnp.float32), held, held),
        in_specs=[VMEM] * 9,
        out_specs=(HBM,) * 3,
        scratch_shapes=[pltpu.VMEM((columns, width), jnp.float32), pltpu.SemaphoreType.DMA((6,))],
        compiler_params=limit(8),
        name="back",
    )(steps, first_new, second_new, own, other_0, pair, other_pair, blocks[3], other_3)


def solution(mesh):
    finer = Mesh(mesh.devices.reshape(4, 16, 2, 4), ("x", "z", "c", "y"))
    spec = P(FSDP, "y")
    return jax.shard_map(
        step, mesh=finer, in_specs=(spec,) * 4, out_specs=(spec,) * 3, check_vma=False
    )
```

```python
import jax
import jax.numpy as jnp
from jax import lax
from jax.experimental import pallas as pl
from jax.experimental.pallas import tpu as pltpu
from jax.sharding import Mesh
from jax.sharding import PartitionSpec as P


STEP = 10
FSDP = ("x", "z", "c")
VMEM = pl.BlockSpec(memory_space=pltpu.VMEM)
ROTATED = [[4 * x + (x + d) % 4 for d in range(4)] for x in range(4)]
BOTH = [[(2 * x + c) * 4 + (x + d) % 4 for d in range(4) for c in range(2)] for x in range(4)]


def exchange(parts):
    return lax.all_to_all(parts, ("x", "y"), 0, 0, axis_index_groups=ROTATED, tiled=True)


def exchange_both(parts):
    return lax.all_to_all(parts, ("x", "c", "y"), 0, 0, axis_index_groups=BOTH, tiled=True)


def encode(part):
    scaled = part * 2.0**22
    square = scaled * scaled
    return jnp.where(part < 0.0, -square * square, square * square).astype(jnp.bfloat16)


def decode(sent):
    fourth = sent.astype(jnp.float32)
    size = jnp.sqrt(jnp.sqrt(jnp.abs(fourth))) * 2.0**-22
    return jnp.where(fourth < 0.0, -size, size)


def project(own, swapped, rows, parts):
    for k, grad in enumerate((own, swapped)):
        parts[k] = encode(
            lax.dot_general(
                grad[...], rows, (((1,), (1,)), ((), ())), preferred_element_type=jnp.float32
            )
        )


def first_block(own, swapped, rows, parts):
    project(own, swapped, rows[...], parts)


def middle_block(own, swapped, rows, parts):
    project(own, swapped, rows[...], parts)


def last_blocks(own, swapped, rows_1, rows_2, parts_0, parts_3, out, pair, held):
    core = lax.axis_index("c")
    rows = jnp.concatenate([rows_1[...], rows_2[...]], axis=0)
    pair[...] = rows
    project(own, swapped, rows, held)
    for k in range(2):
        slot = jnp.bitwise_xor(core, k)
        out[slot] = parts_0[k]
        out[slot + 2] = held[k, :, :128]
        out[slot + 4] = held[k, :, 128:]
        out[slot + 6] = parts_3[k]


def moments(received, first, second, first_out, second_out, copies):
    at = lax.broadcasted_iota(jnp.int32, (256, 256), 0)
    rank = lax.broadcasted_iota(jnp.int32, (256, 256), 1)
    core = lax.axis_index("c")
    half = jnp.bitwise_xor(lax.shift_right_logical(at, 7), core)
    spot = (lax.shift_right_logical(at, 3) & 15) * 16 + half * 8 + (at & 7)
    place = (rank == spot).astype(jnp.bfloat16)
    halves = []
    for k in range(2):
        slot = jnp.bitwise_xor(core, k)
        halves.append(sum(decode(received[slot + 2 * d]) for d in range(4)))
    left = jnp.concatenate(halves, axis=1)
    projected = jnp.zeros(first.shape, jnp.float32)
    for _ in range(3):
        piece = left.astype(jnp.bfloat16)
        projected += jnp.dot(piece, place, preferred_element_type=jnp.float32)
        left = left - piece.astype(jnp.float32)
    first_new = 0.9 * first[...] + 0.1 * projected
    second_new = 0.999 * second[...] + 0.001 * projected * projected
    first_out[...] = first_new
    second_out[...] = second_new
    correct_one = 1.0 - 0.9**STEP
    correct_two = 1.0 - 0.999**STEP
    normalized = (first_new / correct_one / (jnp.sqrt(second_new / correct_two) + 1e-08)).astype(
        jnp.bfloat16
    )
    turned = lax.dot_general(
        normalized, place, (((1,), (1,)), ((), ())), preferred_element_type=jnp.float32
    ).astype(jnp.bfloat16)
    for k in range(4):
        copies[k] = turned


def back(steps, first, second, *refs):
    (own_0, other_0, pair, other_pair, own_3, other_3), refs = refs[:6], refs[6:]
    out, first_out, second_out, held, sems = refs
    low, high = pl.ds(0, 128), pl.ds(128, 128)
    width = 512
    sent = [
        pltpu.make_async_copy(first, first_out, sems.at[4]),
        pltpu.make_async_copy(second, second_out, sems.at[5]),
    ]
    for copy in sent:
        copy.start()
    for k in range(4):
        columns = pl.ds(k * width, width)
        total = jnp.zeros((steps.shape[1], width), jnp.float32)
        for d, (one, two, where) in enumerate(
            (
                (own_0, other_0, low),
                (pair, other_pair, low),
                (pair, other_pair, high),
                (own_3, other_3, low),
            )
        ):
            rows = jnp.concatenate([one[where, columns], two[where, columns]], axis=0)
            total += jnp.dot(steps[d], rows, preferred_element_type=jnp.float32)
        held[:, columns] = total
        copy = pltpu.make_async_copy(held.at[:, columns], out.at[:, columns], sems.at[k])
        copy.start()
        sent.append(copy)
    for copy in sent:
        copy.wait()


def limit(mib):
    return pltpu.CompilerParams(vmem_limit_bytes=mib * 2**20)


def call(kernel, out_shape, *operands):
    many = isinstance(out_shape, tuple)
    return pl.pallas_call(
        kernel,
        out_shape=out_shape,
        in_specs=[VMEM] * len(operands),
        out_specs=(VMEM,) * len(out_shape) if many else VMEM,
        compiler_params=limit(8),
    )(*operands)


def step(grad, projector_t, first_moment, second_moment):
    own = lax.all_gather(projector_t, "z", axis=0, tiled=True)

    def from_x(d):
        return lax.ppermute(own, "x", [(x, (x - d) % 4) for x in range(4)])

    def from_core(block):
        return lax.ppermute(block, "c", [(0, 1), (1, 0)])

    blocks = {0: own}
    for d in (1, 3, 2):
        blocks[d] = from_x(d)
    other_0 = from_core(blocks[0])
    other_3 = from_core(blocks[3])
    columns, ranks = first_moment.shape
    two = jax.ShapeDtypeStruct((2, columns, ranks // 2), jnp.bfloat16)
    eight = jax.ShapeDtypeStruct((8, columns, ranks // 2), jnp.bfloat16)
    four = jax.ShapeDtypeStruct((4, columns, ranks), jnp.bfloat16)
    held = jax.ShapeDtypeStruct((columns, ranks), jnp.float32)
    swapped = lax.ppermute(grad, "c", [(0, 1), (1, 0)])
    parts_0 = call(first_block, two, grad, swapped, blocks[0])
    parts_3 = call(middle_block, two, grad, swapped, blocks[3])
    parts, pair = pl.pallas_call(
        last_blocks,
        out_shape=(eight, jax.ShapeDtypeStruct((256, grad.shape[1]), jnp.bfloat16)),
        in_specs=[VMEM] * 6,
        out_specs=(VMEM,) * 2,
        scratch_shapes=[pltpu.VMEM((2, columns, ranks), jnp.bfloat16)],
        compiler_params=limit(8),
        name="last_blocks",
    )(grad, swapped, blocks[1], blocks[2], parts_0, parts_3)
    other_pair = from_core(pair)
    received = exchange_both(parts)
    first_new, second_new, copies = call(
        moments, (held, held, four), received, first_moment, second_moment
    )
    steps = exchange(copies)
    width = projector_t.shape[1]
    HBM = pl.BlockSpec(memory_space=pl.ANY)
    return pl.pallas_call(
        back,
        out_shape=(jax.ShapeDtypeStruct((columns, width), jnp.float32), held, held),
        in_specs=[VMEM] * 9,
        out_specs=(HBM,) * 3,
        scratch_shapes=[pltpu.VMEM((columns, width), jnp.float32), pltpu.SemaphoreType.DMA((6,))],
        compiler_params=limit(8),
        name="back",
    )(steps, first_new, second_new, own, other_0, pair, other_pair, blocks[3], other_3)


def solution(mesh):
    finer = Mesh(mesh.devices.reshape(4, 16, 2, 4), ("x", "z", "c", "y"))
    spec = P(FSDP, "y")
    return jax.shard_map(
        step, mesh=finer, in_specs=(spec,) * 4, out_specs=(spec,) * 3, check_vma=False
    )
```

```python
import jax
import jax.numpy as jnp
from jax import lax
from jax.experimental import pallas as pl
from jax.experimental.pallas import tpu as pltpu
from jax.sharding import Mesh
from jax.sharding import PartitionSpec as P


STEP = 10
FSDP = ("x", "z", "c")
VMEM = pl.BlockSpec(memory_space=pltpu.VMEM)
ROTATED = [[4 * x + (x + d) % 4 for d in range(4)] for x in range(4)]
BOTH = [[(2 * x + c) * 4 + (x + d) % 4 for d in range(4) for c in range(2)] for x in range(4)]


def exchange(parts):
    return lax.all_to_all(parts, ("x", "y"), 0, 0, axis_index_groups=ROTATED, tiled=True)


def exchange_both(parts):
    return lax.all_to_all(parts, ("x", "c", "y"), 0, 0, axis_index_groups=BOTH, tiled=True)


def encode(part):
    scaled = part * 2.0**22
    square = scaled * scaled
    return jnp.where(part < 0.0, -square * square, square * square).astype(jnp.bfloat16)


def decode(sent):
    fourth = sent.astype(jnp.float32)
    size = jnp.sqrt(jnp.sqrt(jnp.abs(fourth))) * 2.0**-22
    return jnp.where(fourth < 0.0, -size, size)


def project(own, swapped, rows, parts):
    for k, grad in enumerate((own, swapped)):
        parts[k] = encode(
            lax.dot_general(
                grad[...], rows, (((1,), (1,)), ((), ())), preferred_element_type=jnp.float32
            )
        )


def first_block(own, swapped, rows, parts):
    project(own, swapped, rows[...], parts)


def middle_block(own, swapped, rows, parts):
    project(own, swapped, rows[...], parts)


def last_blocks(own, swapped, rows_1, rows_2, parts_0, parts_3, out, pair, held):
    core = lax.axis_index("c")
    rows = jnp.concatenate([rows_1[...], rows_2[...]], axis=0)
    pair[...] = rows
    project(own, swapped, rows, held)
    for k in range(2):
        slot = jnp.bitwise_xor(core, k)
        out[slot] = parts_0[k]
        out[slot + 2] = held[k, :, :128]
        out[slot + 4] = held[k, :, 128:]
        out[slot + 6] = parts_3[k]


def moments(received, first, second, first_out, second_out, copies):
    at = lax.broadcasted_iota(jnp.int32, (256, 256), 0)
    rank = lax.broadcasted_iota(jnp.int32, (256, 256), 1)
    core = lax.axis_index("c")
    half = jnp.bitwise_xor(lax.shift_right_logical(at, 7), core)
    spot = (lax.shift_right_logical(at, 3) & 15) * 16 + half * 8 + (at & 7)
    place = (rank == spot).astype(jnp.bfloat16)
    projected = jnp.zeros(first.shape, jnp.float32)
    for d in range(4):
        both = [received[jnp.bitwise_xor(core, k) + 2 * d] for k in range(2)]
        moved = jnp.dot(
            jnp.concatenate(both, axis=1), place, preferred_element_type=jnp.float32
        )
        projected += decode(moved)
    first_new = 0.9 * first[...] + 0.1 * projected
    second_new = 0.999 * second[...] + 0.001 * projected * projected
    first_out[...] = first_new
    second_out[...] = second_new
    correct_one = 1.0 - 0.9**STEP
    correct_two = 1.0 - 0.999**STEP
    normalized = (first_new / correct_one / (jnp.sqrt(second_new / correct_two) + 1e-08)).astype(
        jnp.bfloat16
    )
    turned = lax.dot_general(
        normalized, place, (((1,), (1,)), ((), ())), preferred_element_type=jnp.float32
    ).astype(jnp.bfloat16)
    for k in range(4):
        copies[k] = turned


def back(steps, first, second, *refs):
    (own_0, other_0, pair, other_pair, own_3, other_3), refs = refs[:6], refs[6:]
    out, first_out, second_out, held, sems = refs
    low, high = pl.ds(0, 128), pl.ds(128, 128)
    width = 512
    sent = [
        pltpu.make_async_copy(first, first_out, sems.at[4]),
        pltpu.make_async_copy(second, second_out, sems.at[5]),
    ]
    for copy in sent:
        copy.start()
    for k in range(4):
        columns = pl.ds(k * width, width)
        total = jnp.zeros((steps.shape[1], width), jnp.float32)
        for d, (one, two, where) in enumerate(
            (
                (own_0, other_0, low),
                (pair, other_pair, low),
                (pair, other_pair, high),
                (own_3, other_3, low),
            )
        ):
            rows = jnp.concatenate([one[where, columns], two[where, columns]], axis=0)
            total += jnp.dot(steps[d], rows, preferred_element_type=jnp.float32)
        held[:, columns] = total
        copy = pltpu.make_async_copy(held.at[:, columns], out.at[:, columns], sems.at[k])
        copy.start()
        sent.append(copy)
    for copy in sent:
        copy.wait()


def limit(mib):
    return pltpu.CompilerParams(vmem_limit_bytes=mib * 2**20)


def call(kernel, out_shape, *operands):
    many = isinstance(out_shape, tuple)
    return pl.pallas_call(
        kernel,
        out_shape=out_shape,
        in_specs=[VMEM] * len(operands),
        out_specs=(VMEM,) * len(out_shape) if many else VMEM,
        compiler_params=limit(8),
    )(*operands)


def step(grad, projector_t, first_moment, second_moment):
    own = lax.all_gather(projector_t, "z", axis=0, tiled=True)

    def from_x(d):
        return lax.ppermute(own, "x", [(x, (x - d) % 4) for x in range(4)])

    def from_core(block):
        return lax.ppermute(block, "c", [(0, 1), (1, 0)])

    blocks = {0: own}
    for d in (1, 3, 2):
        blocks[d] = from_x(d)
    other_0 = from_core(blocks[0])
    other_3 = from_core(blocks[3])
    columns, ranks = first_moment.shape
    two = jax.ShapeDtypeStruct((2, columns, ranks // 2), jnp.bfloat16)
    eight = jax.ShapeDtypeStruct((8, columns, ranks // 2), jnp.bfloat16)
    four = jax.ShapeDtypeStruct((4, columns, ranks), jnp.bfloat16)
    held = jax.ShapeDtypeStruct((columns, ranks), jnp.float32)
    swapped = lax.ppermute(grad, "c", [(0, 1), (1, 0)])
    parts_0 = call(first_block, two, grad, swapped, blocks[0])
    parts_3 = call(middle_block, two, grad, swapped, blocks[3])
    parts, pair = pl.pallas_call(
        last_blocks,
        out_shape=(eight, jax.ShapeDtypeStruct((256, grad.shape[1]), jnp.bfloat16)),
        in_specs=[VMEM] * 6,
        out_specs=(VMEM,) * 2,
        scratch_shapes=[pltpu.VMEM((2, columns, ranks), jnp.bfloat16)],
        compiler_params=limit(8),
        name="last_blocks",
    )(grad, swapped, blocks[1], blocks[2], parts_0, parts_3)
    other_pair = from_core(pair)
    received = exchange_both(parts)
    first_new, second_new, copies = call(
        moments, (held, held, four), received, first_moment, second_moment
    )
    steps = exchange(copies)
    width = projector_t.shape[1]
    HBM = pl.BlockSpec(memory_space=pl.ANY)
    return pl.pallas_call(
        back,
        out_shape=(jax.ShapeDtypeStruct((columns, width), jnp.float32), held, held),
        in_specs=[VMEM] * 9,
        out_specs=(HBM,) * 3,
        scratch_shapes=[pltpu.VMEM((columns, width), jnp.float32), pltpu.SemaphoreType.DMA((6,))],
        compiler_params=limit(8),
        name="back",
    )(steps, first_new, second_new, own, other_0, pair, other_pair, blocks[3], other_3)


def solution(mesh):
    finer = Mesh(mesh.devices.reshape(4, 16, 2, 4), ("x", "z", "c", "y"))
    spec = P(FSDP, "y")
    return jax.shard_map(
        step, mesh=finer, in_specs=(spec,) * 4, out_specs=(spec,) * 3, check_vma=False
    )
```
